32 devices in a mesh: mem: 2 (over core), row: 8 (over z, y), col: 2 (over x).
Axes of the slice: x: 2, y: 2, z: 4, core: 2. Of those that a mesh axis runs over, the one named last changes fastest.
Arguments:
- tokens: bfloat16 [1024, 2560], P('row', ('mem', 'col')), may hold values from -6 to 6
- cotangent: bfloat16 [1024, 2560], P('row', ('mem', 'col')), may hold values from -3 to 3
- inner_weight: float32 [2, 2560, 6912], P(None, 'row', ('mem', 'col')), may hold values from -0.125 to 0.125
- inner_mean: float32 [2, 2560, 6912], P(None, 'row', ('mem', 'col')), may hold values from -12 to 12
- inner_square: float32 [2, 2560, 6912], P(None, 'row', ('mem', 'col')), may hold values from 2 to 128
- outer_weight: float32 [6912, 2560], P(('mem', 'col'), 'row'), may hold values from -0.078125 to 0.078125
- outer_mean: float32 [6912, 2560], P(('mem', 'col'), 'row'), may hold values from -12 to 12
- outer_square: float32 [6912, 2560], P(('mem', 'col'), 'row'), may hold values from 2 to 128
Outputs:
- token_gradient: bfloat16 [1024, 2560], P('row', ('mem', 'col'))
- inner_stepped: float32 [2, 2560, 6912], P(None, 'row', ('mem', 'col'))
- inner_averaged: float32 [2, 2560, 6912], P(None, 'row', ('mem', 'col'))
- inner_squared: float32 [2, 2560, 6912], P(None, 'row', ('mem', 'col'))
- outer_stepped: float32 [6912, 2560], P(('mem', 'col'), 'row')
- outer_averaged: float32 [6912, 2560], P(('mem', 'col'), 'row')
- outer_squared: float32 [6912, 2560], P(('mem', 'col'), 'row')
The draws below stay inside these ranges and needn't reach their ends.
All inputs are finite; a program needn't handle non-finite values.
Results may differ from the reference program's by a relative error of at most 0.0072.
Values may be sent and summed in bfloat16 or wider, within the bound.
No kernel may reach another device: no remote copies, remote signals or barrier semaphores. Data moves between devices by JAX's collectives and lax.ppermute only.
A program may use at most 128 MiB of HBM per device.

```python
import math
import jax
import jax.numpy as jnp

D = 2560
FF = 6912
TOKENS = 1024


def with_spikes(drawn, key, source, target, shards_of, factor):
    owner, partner = [(jnp.arange(drawn.shape[axis_at]) // (drawn.shape[axis_at] // shards_of)).reshape([-1 if axis == axis_at else 1 for axis in range(drawn.ndim)]) for axis_at in (source, target)]
    chosen = jax.random.permutation(key, shards_of)[partner]
    strong = (owner == chosen) | (owner == (partner + shards_of // 2) % shards_of)
    return jnp.where(strong, factor * drawn, drawn)


def block_levels(stream_key, shape, pieces, least, largest):
    factor_of, own = 1.0, jax.random.fold_in(stream_key, 6)
    for axis_at, blocks in pieces:
        heights = jnp.exp(jax.random.uniform(jax.random.fold_in(own, axis_at), (blocks,), jnp.float32, least / len(pieces), largest / len(pieces)))
        factor_of = factor_of * jnp.repeat(heights, shape[axis_at] // blocks).reshape([-1 if axis == axis_at else 1 for axis in range(len(shape))])
    return factor_of


def normal_values(stream_key, dims, scale, bound, cuts=(), kind=jnp.bfloat16):
    array = jax.random.normal(stream_key, dims, jnp.float32) * scale
    if len(cuts) > 0:
        array = block_levels(stream_key, dims, cuts, -0.22, 0.18) * array
    return jnp.clip(array, min=-bound, max=bound).astype(kind)


def gaussian_with(rng, extent, deviation, most, shards, heavy, held_as=jnp.bfloat16):
    entries = deviation * jax.random.normal(rng, extent, jnp.float32)
    if shards:
        entries = entries * block_levels(rng, extent, shards, -0.22, 0.18)
    return jnp.clip(with_spikes(entries, jax.random.fold_in(rng, 3), *heavy), -most, most).astype(held_as)


def setup_inputs(seed: int = 0) -> dict:
    key_of = jax.random.split(jax.random.key(seed), 9)
    tokens = gaussian_with(key_of[0], (TOKENS, D), 1.0, 6.0, ((0, 8), (1, 4)), (0, 1, 8, 2.0))
    cotangent = gaussian_with(key_of[1], (TOKENS, D), 0.5, 3.0, ((0, 8), (1, 4)), (0, 1, 8, 2.0))
    inner_weight = normal_values(key_of[2], (2, D, FF), D ** -0.5, 0.125, ((1, 8), (2, 4)), jnp.float32)
    inner_mean = normal_values(key_of[3], (2, D, FF), 2.0, 12.0, ((1, 8), (2, 4)), jnp.float32)
    inner_square = jnp.clip(jnp.exp(math.log(128.0) - 4.158883 * jax.random.uniform(key_of[4], (2, D, FF), jnp.float32) ** block_levels(key_of[4], (2, D, FF), ((1, 8), (2, 4)), -0.2, 0.2)), 2.0, 128.0)
    outer_weight = normal_values(key_of[5], (FF, D), FF ** -0.5, 0.078125, ((0, 4), (1, 8)), jnp.float32)
    outer_mean = normal_values(key_of[6], (FF, D), 2.0, 12.0, ((0, 4), (1, 8)), jnp.float32)
    outer_square = jnp.clip(jnp.exp(math.log(128.0) - 4.158883 * jax.random.uniform(key_of[7], (FF, D), jnp.float32) ** block_levels(key_of[7], (FF, D), ((0, 4), (1, 8)), -0.2, 0.2)), 2.0, 128.0)
    return {"tokens": tokens, "cotangent": cotangent, "inner_weight": inner_weight, "inner_mean": inner_mean, "inner_square": inner_square, "outer_weight": outer_weight, "outer_mean": outer_mean, "outer_square": outer_square}


beta_one = 0.9
beta_two = 0.95
learn_rate = 0.01
weight_decay = 0.1
epsilon = 1e-08
bias_steps = 20.0

def adam_step(weight, moment, square, gradient):
    moment_next = beta_one * moment + (1.0 - beta_one) * gradient
    square_next = beta_two * square + (1.0 - beta_two) * gradient * gradient
    scaled_moment = moment_next / (1.0 - beta_one ** bias_steps)
    scaled_square = square_next / (1.0 - beta_two ** bias_steps)
    change = scaled_moment / (jnp.sqrt(scaled_square) + epsilon) + weight_decay * weight
    return (weight - learn_rate * change, moment_next, square_next)

def reference(tokens, cotangent, inner_weight, inner_mean, inner_square, outer_weight, outer_mean, outer_square):
    inner_low = inner_weight.astype(jnp.bfloat16)
    outer_low = outer_weight.astype(jnp.bfloat16)
    gating = jnp.dot(tokens, inner_low[0], preferred_element_type=jnp.float32)
    upward = jnp.dot(tokens, inner_low[1], preferred_element_type=jnp.float32)
    logistic = jax.nn.sigmoid(gating)
    hidden = (gating * logistic * upward).astype(jnp.bfloat16)
    hidden_back = jnp.dot(cotangent, outer_low.T, preferred_element_type=jnp.float32)
    gating_back = (hidden_back * upward * logistic * (1.0 + gating * (1.0 - logistic))).astype(jnp.bfloat16)
    upward_back = (hidden_back * gating * logistic).astype(jnp.bfloat16)
    token_gradient = (jnp.dot(gating_back, inner_low[0].T, preferred_element_type=jnp.float32) + jnp.dot(upward_back, inner_low[1].T, preferred_element_type=jnp.float32)).astype(jnp.bfloat16)
    inner_grad = jnp.stack([jnp.dot(tokens.T, gating_back, preferred_element_type=jnp.float32), jnp.dot(tokens.T, upward_back, preferred_element_type=jnp.float32)])
    outer_grad = jnp.dot(hidden.T, cotangent, preferred_element_type=jnp.float32)
    inner_stepped, inner_averaged, inner_squared = adam_step(inner_weight, inner_mean, inner_square, inner_grad)
    outer_stepped, outer_averaged, outer_squared = adam_step(outer_weight, outer_mean, outer_square, outer_grad)
    return (token_gradient, inner_stepped, inner_averaged, inner_squared, outer_stepped, outer_averaged, outer_squared)
```

```python
import jax
import jax.numpy as jnp
from jax import lax
from jax.sharding import PartitionSpec as P


beta_one = 0.9
beta_two = 0.95
learn_rate = 0.01
weight_decay = 0.1
epsilon = 1e-08
bias_steps = 20.0
bf16 = jnp.bfloat16
f32 = jnp.float32


def contract(left_side, right_side, left_axis, right_axis):
    return lax.dot_general(
        left_side,
        right_side,
        (((left_axis,), (right_axis,)), ((), ())),
        preferred_element_type=f32,
    )


def adam_step(weight, moment, square, gradient):
    moment_next = beta_one * moment + (1.0 - beta_one) * gradient
    square_next = beta_two * square + (1.0 - beta_two) * gradient * gradient
    scaled_moment = moment_next / (1.0 - beta_one**bias_steps)
    scaled_square = square_next / (1.0 - beta_two**bias_steps)
    change = scaled_moment / (jnp.sqrt(scaled_square) + epsilon) + weight_decay * weight
    return (weight - learn_rate * change, moment_next, square_next)


def build(mesh):
    n_row, n_col, n_mem = (mesh.shape[name] for name in ("row", "col", "mem"))
    n_z = n_col * n_mem
    n_y = n_row // n_z
    assert n_y * n_z == n_row

    def send_row(block, step_z, step_y):
        pairs = []
        for z in range(n_z):
            for y in range(n_y):
                target = ((z + step_z) % n_z) * n_y + (y + step_y) % n_y
                pairs.append((z * n_y + y, target))
        return lax.ppermute(block, "row", pairs)

    def send(block, name, step):
        count = mesh.shape[name]
        return lax.ppermute(block, name, [(i, (i + step) % count) for i in range(count)])

    def exchange_z(blocks):
        out = [None] * n_z
        out[0] = blocks[0]
        if n_z == 4:
            half = blocks[2].shape[-2] // 2
            there = send_row(blocks[2][..., :half, :], 1, 0)
            back = send_row(blocks[2][..., half:, :], -1, 0)
            out[3] = send_row(blocks[1], 1, 0)
            out[1] = send_row(blocks[3], -1, 0)
            there = send_row(there, 1, 0)
            back = send_row(back, -1, 0)
            out[2] = jnp.concatenate([there, back], axis=-2)
        else:
            for k in range(1, n_z):
                out[n_z - k] = send_row(blocks[k], k, 0)
        return out

    def gather_z(block):
        out = [None] * n_z
        out[0] = block
        if n_z == 4:
            half = block.shape[-2] // 2
            out[1] = send_row(block, -1, 0)
            out[3] = send_row(block, 1, 0)
            there = send_row(out[1][..., :half, :], -1, 0)
            back = send_row(out[3][..., half:, :], 1, 0)
            out[2] = jnp.concatenate([there, back], axis=-2)
        else:
            for k in range(1, n_z):
                out[k] = send_row(block, -k, 0)
        return out

    def gather_y(block):
        return [block] + [send_row(block, 0, -e) for e in range(1, n_y)]

    def gather_name(block, name):
        return [block] + [send(block, name, -s) for s in range(1, mesh.shape[name])]

    def pick(stack, index, axis=0):
        return lax.dynamic_index_in_dim(stack, index, axis, keepdims=False)

    def exchange_row(packed, at_z, at_y):
        first = (packed.shape[2] // 2) // 8 * 8
        parts = []
        for e in range(n_y):
            kept = pick(packed[:, :, :first], (at_y + e) % n_y, 1)
            parts.append(kept if e == 0 else send_row(kept, 0, e))
        parts = [parts[(-e) % n_y] for e in range(n_y)]
        stacked = jnp.stack(parts, axis=1)
        one = exchange_z([pick(stacked, (at_z + k) % n_z) for k in range(n_z)])
        one = jnp.stack(one, axis=0)
        two = exchange_z([pick(packed[:, :, first:], (at_z + k) % n_z) for k in range(n_z)])
        two = jnp.stack(two, axis=0)
        parts = []
        for e in range(n_y):
            kept = pick(two, (at_y + e) % n_y, 1)
            parts.append(kept if e == 0 else send_row(kept, 0, e))
        parts = [parts[(-e) % n_y] for e in range(n_y)]
        two = jnp.stack(parts, axis=1)
        return jnp.concatenate([one, two], axis=2)

    def on_device(
        tokens,
        cotangent,
        inner_weight,
        inner_mean,
        inner_square,
        outer_weight,
        outer_mean,
        outer_square,
    ):
        row = lax.axis_index("row")
        at_z, at_y = row // n_y, row % n_y
        at_m, at_x = lax.axis_index("mem"), lax.axis_index("col")
        token_count, slab = tokens.shape
        width, hidden_local = inner_weight.shape[1:]
        share = hidden_local // n_row

        packed = jnp.concatenate(
            [
                inner_weight[0].T.astype(bf16),
                inner_weight[1].T.astype(bf16),
                outer_weight.astype(bf16),
            ],
            axis=1,
        ).reshape(n_z, n_y, share, 3 * width)
        weights = exchange_row(packed, at_z, at_y)

        held = jnp.stack(gather_y(tokens))
        held = jnp.stack(gather_z(held))
        token_slab = held.reshape(n_row * token_count, slab)
        held = jnp.stack(gather_z(cotangent))
        held = jnp.stack(gather_y(held), axis=1)
        cotangent_slab = held.reshape(n_row * token_count, slab)

        def spread(block):
            blocks = gather_name(block, "col")
            across = [gather_name(b, "mem") for b in blocks]
            return [across[b][a] for a in range(n_mem) for b in range(n_col)]

        token_slabs, cotangent_slabs = spread(token_slab), spread(cotangent_slab)

        def slab_at(a, b):
            return ((at_m + a) % n_mem) * n_col + (at_x + b) % n_col

        gate_w, up_w, out_w = [], [], []
        for a in range(n_mem):
            for b in range(n_col):
                from_z = pick(weights, (slab_at(a, b) - at_z) % n_z)
                halves = [pick(from_z, (y - at_y) % n_y) for y in range(n_y)]
                for i, target in enumerate((gate_w, up_w, out_w)):
                    target.append(
                        jnp.concatenate([h[:, i * width : (i + 1) * width] for h in halves], axis=1)
                    )

        def summed(ws, xs):
            total = contract(ws[0], xs[0], 1, 1)
            for w, x in zip(ws[1:], xs[1:]):
                total = total + contract(w, x, 1, 1)
            return total

        gating = summed(gate_w, token_slabs)
        upward = summed(up_w, token_slabs)
        hidden_back = summed(out_w, cotangent_slabs)
        logistic = jax.nn.sigmoid(gating)
        hidden = (gating * logistic * upward).astype(bf16)
        gating_back = (
            hidden_back * upward * logistic * (1.0 + gating * (1.0 - logistic))
        ).astype(bf16)
        upward_back = (hidden_back * gating * logistic).astype(bf16)

        both = jnp.concatenate([gating_back, upward_back], axis=0)
        partial = [
            contract(both, jnp.concatenate([g, u], axis=0), 0, 0) for g, u in zip(gate_w, up_w)
        ]
        sums = []
        for b in range(n_col):
            total = partial[b]
            for a in range(1, n_mem):
                total = total + send(partial[a * n_col + b].astype(bf16), "mem", a).astype(f32)
            sums.append(total)
        total = sums[0]
        for b in range(1, n_col):
            total = total + send(sums[b].astype(bf16), "col", b).astype(f32)
        total = total.reshape(n_z, n_y, token_count, slab)
        mine = total[:, 0]
        for e in range(1, n_y):
            mine = mine + send_row(total[:, e].astype(bf16), 0, e).astype(f32)
        pieces = exchange_z([mine[k].astype(bf16) for k in range(n_z)])
        token_gradient = mine[0]
        for k in range(1, n_z):
            token_gradient = token_gradient + pieces[k].astype(f32)
        token_gradient = token_gradient.astype(bf16)

        slabs = []
        for t, c in zip(token_slabs, cotangent_slabs):
            g = contract(gating_back, t, 1, 0).astype(bf16)
            u = contract(upward_back, t, 1, 0).astype(bf16)
            o = contract(hidden, c, 1, 0).astype(bf16)
            slabs.append(
                jnp.stack(
                    [
                        jnp.concatenate(
                            [v[:, y * width : (y + 1) * width] for v in (g, u, o)], axis=1
                        )
                        for y in range(n_y)
                    ]
                )
            )
        slabs = jnp.stack(slabs)
        packed = jnp.stack(
            [
                pick(slabs, ((z // n_col - at_m) % n_mem) * n_col + (z % n_col - at_x) % n_col)
                for z in range(n_z)
            ]
        )
        back = exchange_row(packed, at_z, at_y)
        gradient = jnp.stack(
            [
                pick(pick(back, (z - at_z) % n_z), (y - at_y) % n_y)
                for z in range(n_z)
                for y in range(n_y)
            ]
        ).reshape(hidden_local, 3 * width)
        inner_gradient = jnp.stack(
            [gradient[:, :width].T, gradient[:, width : 2 * width].T]
        ).astype(f32)
        outer_gradient = gradient[:, 2 * width :].astype(f32)
        return (
            token_gradient,
            *adam_step(inner_weight, inner_mean, inner_square, inner_gradient),
            *adam_step(outer_weight, outer_mean, outer_square, outer_gradient),
        )

    return on_device


def solution(mesh):
    activation = P("row", ("mem", "col"))
    inner = P(None, "row", ("mem", "col"))
    outer = P(("mem", "col"), "row")
    return jax.shard_map(
        build(mesh),
        mesh=mesh,
        in_specs=(activation, activation, inner, inner, inner, outer, outer, outer),
        out_specs=(activation, inner, inner, inner, outer, outer, outer),
        check_vma=False,
    )
```

```python
import functools

import jax
import jax.numpy as jnp
from jax import lax
from jax.experimental import pallas as pl
from jax.experimental.pallas import tpu as pltpu
from jax.sharding import PartitionSpec as P


beta_one = 0.9
beta_two = 0.95
learn_rate = 0.01
weight_decay = 0.1
epsilon = 1e-08
bias_steps = 20.0
bf16 = jnp.bfloat16
f32 = jnp.float32


def contract(left_side, right_side, left_axis, right_axis):
    return lax.dot_general(
        left_side,
        right_side,
        (((left_axis,), (right_axis,)), ((), ())),
        preferred_element_type=f32,
    )


def adam_step(weight, moment, square, gradient):
    moment_next = beta_one * moment + (1.0 - beta_one) * gradient
    square_next = beta_two * square + (1.0 - beta_two) * gradient * gradient
    scaled_moment = moment_next * (1.0 / (1.0 - beta_one**bias_steps))
    scaled_square = square_next * (1.0 / (1.0 - beta_two**bias_steps))
    change = scaled_moment / (jnp.sqrt(scaled_square) + epsilon) + weight_decay * weight
    return (weight - learn_rate * change, moment_next, square_next)


lanes = 256


def pack_kernel(weight_ref, packed_ref):
    pair, width, block = weight_ref.shape
    packed_ref[...] = weight_ref[...].reshape(pair * width, block).T.astype(bf16)


def pack(weight):
    pair, width, hidden = weight.shape
    return pl.pallas_call(
        pack_kernel,
        grid=(pl.cdiv(hidden, lanes),),
        in_specs=[pl.BlockSpec((pair, width, lanes), lambda i: (0, 0, i))],
        out_specs=pl.BlockSpec((lanes, pair * width), lambda i: (i, 0)),
        out_shape=jax.ShapeDtypeStruct((hidden, pair * width), bf16),
        cost_estimate=pl.CostEstimate(
            flops=20 * weight.size, bytes_accessed=6 * weight.size, transcendentals=0
        ),
        name="pack",
    )(weight)


def adam_kernel(weight_ref, mean_ref, square_ref, gradient_ref, *out_refs):
    gradient = gradient_ref[...].astype(f32).T.reshape(weight_ref.shape)
    results = adam_step(weight_ref[...], mean_ref[...], square_ref[...], gradient)
    for out_ref, result in zip(out_refs, results):
        out_ref[...] = result


def adam_transposed(weight, mean, square, gradient):
    pair, width, hidden = weight.shape
    spec = pl.BlockSpec((pair, width, lanes), lambda i: (0, 0, i))
    return pl.pallas_call(
        adam_kernel,
        grid=(pl.cdiv(hidden, lanes),),
        in_specs=[spec] * 3 + [pl.BlockSpec((lanes, pair * width), lambda i: (i, 0))],
        out_specs=[spec] * 3,
        out_shape=[jax.ShapeDtypeStruct(weight.shape, f32)] * 3,
        cost_estimate=pl.CostEstimate(
            flops=20 * weight.size, bytes_accessed=26 * weight.size, transcendentals=weight.size
        ),
        name="adam",
    )(weight, mean, square, gradient)


vmem = pl.BlockSpec(memory_space=pltpu.VMEM)
smem = pl.BlockSpec(memory_space=pltpu.SMEM)


def grant(mebibytes):
    return pltpu.CompilerParams(vmem_limit_bytes=mebibytes * 1024 * 1024)


def parts_of(width):
    whole = width // 128 * 128
    return whole, width - whole


def spans(width, y):
    whole, rest = parts_of(width)
    return pl.multiple_of(y * rest, 8), pl.multiple_of((1 - y) * whole, 8)


def piece_columns(width):
    return 3 * parts_of(width)[0] + 256


def pack_pieces_kernel(place_ref, inner_ref, outer_ref, *refs):
    piece_refs, turned_ref = refs[:-1], refs[-1]
    step = pl.program_id(0)
    width, block = outer_ref.shape
    whole, rest = parts_of(width)
    first, second = spans(width, place_ref[0] % 2)
    sources = (inner_ref.at[0], inner_ref.at[1], outer_ref)
    both = jnp.concatenate(
        [ref[pl.ds(first, whole), :] for ref in sources]
        + [ref[pl.ds(second, rest), :] for ref in sources]
        + [jnp.zeros((rest, block), f32)],
        axis=0,
    )
    turned_ref[pl.ds(pl.multiple_of(step * block, block), block), :] = both.T

    @pl.when(step == pl.num_programs(0) - 1)
    def _():
        for i, piece_ref in enumerate(piece_refs):
            share = piece_ref.shape[0]
            start = pl.multiple_of((place_ref[0] ^ i) * share, 8)
            piece_ref[...] = turned_ref[pl.ds(start, share), :].astype(bf16)


def pack_pieces(place, inner, outer_turned, pieces):
    pair, width, hidden = inner.shape
    steps = pl.cdiv(hidden, lanes)
    columns = piece_columns(width)
    shape = jax.ShapeDtypeStruct((hidden // pieces, columns), bf16)
    return pl.pallas_call(
        pack_pieces_kernel,
        grid=(steps,),
        in_specs=[
            smem,
            pl.BlockSpec((pair, width, lanes), lambda i: (0, 0, i)),
            pl.BlockSpec((width, lanes), lambda i: (0, i)),
        ],
        out_specs=[pl.BlockSpec(shape.shape, lambda i: (0, 0))] * pieces,
        out_shape=[shape] * pieces,
        scratch_shapes=[pltpu.VMEM((steps * lanes, columns), f32)],
        compiler_params=grant(18),
        cost_estimate=pl.CostEstimate(
            flops=30 * inner.size, bytes_accessed=9 * inner.size, transcendentals=0
        ),
        name="pack_pieces",
    )(place, inner, outer_turned)


def rest_lanes(width, c):
    whole, rest = parts_of(width)
    return slice(3 * whole + c * rest, 3 * whole + (c + 1) * rest)


def project_kernel(width, place_ref, *refs):
    pieces, refs = refs[:8], refs[8:]
    tokens, cotangents, refs = refs[:4], refs[4:8], refs[8:]
    gating_turned, upward_turned, gating_back_ref, upward_back_ref, hidden_ref = refs[:5]
    weights_ref, held = refs[5:]
    at_z, at_y, at_slab = place_ref[0] // 2, place_ref[0] % 2, place_ref[1]
    whole, rest = parts_of(width)

    for side in range(2):

        @pl.when(at_y == side)
        def _():
            for k in range(4):
                low, high = pieces[2 * k + side], pieces[2 * k + 1 - side]
                for c in range(3):
                    lanes_c, rest_c = slice(c * whole, (c + 1) * whole), rest_lanes(width, c)
                    held[at_z ^ k, c, :, :whole] = low[:, lanes_c]
                    held[at_z ^ k, c, :, whole + 2 * rest :] = high[:, lanes_c]
                    held[at_z ^ k, c, :, whole : whole + 2 * rest] = jnp.concatenate(
                        [low[:, rest_c], high[:, rest_c]], axis=1
                    )

    def product(c, activations):
        total = None
        for j in range(4):
            part = contract(activations[j][...], held[at_slab ^ j, c], 1, 1)
            total = part if total is None else total + part
        return total

    for j in range(4):
        for c in range(2):
            weights_ref[j, c] = held[at_slab ^ j, c]
    hidden_back = product(2, cotangents)
    gating = product(0, tokens)
    upward = product(1, tokens)
    logistic = 1.0 / (1.0 + jnp.exp(-gating))
    hidden = gating * logistic * upward
    gating_back = hidden_back * upward * logistic * (1.0 + gating * (1.0 - logistic))
    upward_back = hidden_back * gating * logistic
    gating_turned[...] = gating_back.astype(bf16)
    upward_turned[...] = upward_back.astype(bf16)
    hidden_ref[...] = hidden.T.astype(bf16)
    gating_back_ref[...] = gating_back.T.astype(bf16)
    upward_back_ref[...] = upward_back.T.astype(bf16)


def project(place, pieces, tokens, cotangents, width):
    share = pieces[0].shape[0]
    rows, slab = tokens[0].shape
    shapes = [
        *[jax.ShapeDtypeStruct((rows, share), bf16)] * 2,
        *[jax.ShapeDtypeStruct((share, rows), bf16)] * 3,
        jax.ShapeDtypeStruct((4, 2, share, slab), bf16),
    ]
    return pl.pallas_call(
        functools.partial(project_kernel, width),
        in_specs=[smem] + [vmem] * 16,
        out_specs=[vmem] * 6,
        out_shape=shapes,
        scratch_shapes=[pltpu.VMEM((4, 3, share, slab), bf16)],
        compiler_params=grant(24),
        cost_estimate=pl.CostEstimate(
            flops=24 * share * rows * slab, bytes_accessed=16 * rows * slab, transcendentals=0
        ),
        name="project",
    )(place, *pieces, *tokens, *cotangents)


def gradient_kernel(width, place_ref, gating_back_ref, upward_back_ref, hidden_ref, *refs):
    tokens, cotangents, outs, held = refs[:4], refs[4:8], refs[8:16], refs[16]
    at_z, at_y, at_slab = place_ref[0] // 2, place_ref[0] % 2, place_ref[1]
    for j in range(4):
        for c, (left, right) in enumerate(
            ((gating_back_ref, tokens), (upward_back_ref, tokens), (hidden_ref, cotangents))
        ):
            held[at_slab ^ j, c] = contract(left[...], right[j][...], 1, 0).astype(bf16)
    whole, rest = parts_of(width)
    for side in range(2):

        @pl.when(at_y == side)
        def _():
            for i in range(8):
                half = side ^ (i % 2)
                first = half * (whole + 2 * rest)
                second = whole + half * rest
                rests = []
                for c in range(3):
                    slab = held.at[at_z ^ (i // 2), c]
                    outs[i][:, c * whole : (c + 1) * whole] = slab[:, first : first + whole]
                    rests.append(slab[:, second : second + rest])
                rests.append(jnp.zeros_like(rests[0]))
                outs[i][:, 3 * whole :] = jnp.concatenate(rests, axis=1)


def gradients(place, gating_back, upward_back, hidden, tokens, cotangents, width):
    share, rows = gating_back.shape
    slab = tokens[0].shape[1]
    return pl.pallas_call(
        functools.partial(gradient_kernel, width),
        in_specs=[smem] + [vmem] * 11,
        out_specs=[vmem] * 8,
        out_shape=[jax.ShapeDtypeStruct((share, piece_columns(width)), bf16)] * 8,
        scratch_shapes=[pltpu.VMEM((4, 3, share, slab), bf16)],
        compiler_params=grant(22),
        cost_estimate=pl.CostEstimate(
            flops=24 * share * rows * slab, bytes_accessed=16 * rows * slab, transcendentals=0
        ),
        name="gradients",
    )(place, gating_back, upward_back, hidden, *tokens, *cotangents)


def adam_pieces_kernel(place_ref, *refs):
    pieces, states, outs, held = refs[:8], refs[8:14], refs[14:20], refs[20]
    step = pl.program_id(0)

    @pl.when(step == 0)
    def _():
        for i, piece in enumerate(pieces):
            share = piece.shape[0]
            start = pl.multiple_of((place_ref[0] ^ i) * share, 8)
            held[pl.ds(start, share), :] = piece[...].astype(f32)

    pair, width, block = states[0].shape
    whole, rest = parts_of(width)
    gradient = held[pl.ds(pl.multiple_of(step * block, block), block), :].T
    first, second = spans(width, place_ref[0] % 2)
    for c in range(3):
        mine = [ref.at[c] if c < pair else ref for ref in (states[:3] if c < pair else states[3:])]
        theirs = [ref.at[c] if c < pair else ref for ref in (outs[:3] if c < pair else outs[3:])]
        for rows, value in (
            (pl.ds(first, whole), gradient[c * whole : (c + 1) * whole]),
            (pl.ds(second, rest), gradient[rest_lanes(width, c)]),
        ):
            results = adam_step(*(ref[rows, :] for ref in mine), value)
            for out_ref, result in zip(theirs, results):
                out_ref[rows, :] = result


def adam_pieces(place, pieces, inner, outer):
    pair, width, hidden = inner[0].shape
    steps = pl.cdiv(hidden, lanes)
    inner_spec = pl.BlockSpec((pair, width, lanes), lambda i: (0, 0, i))
    outer_spec = pl.BlockSpec((width, lanes), lambda i: (0, i))
    return pl.pallas_call(
        adam_pieces_kernel,
        grid=(steps,),
        in_specs=[smem] + [vmem] * 8 + [inner_spec] * 3 + [outer_spec] * 3,
        out_specs=[inner_spec] * 3 + [outer_spec] * 3,
        out_shape=[jax.ShapeDtypeStruct(inner[0].shape, f32)] * 3
        + [jax.ShapeDtypeStruct(outer[0].shape, f32)] * 3,
        scratch_shapes=[pltpu.VMEM((steps * lanes, piece_columns(width)), f32)],
        compiler_params=grant(27),
        cost_estimate=pl.CostEstimate(
            flops=30 * inner[0].size,
            bytes_accessed=39 * inner[0].size,
            transcendentals=2 * inner[0].size,
        ),
        name="adam_pieces",
    )(place, *pieces, *inner, *outer)


def build(mesh):
    n_row, n_col, n_mem = (mesh.shape[name] for name in ("row", "col", "mem"))
    n_z = n_col * n_mem
    n_y = n_row // n_z
    assert n_y * n_z == n_row

    def send_row(block, step_z, step_y):
        pairs = []
        for z in range(n_z):
            for y in range(n_y):
                target = ((z + step_z) % n_z) * n_y + (y + step_y) % n_y
                pairs.append((z * n_y + y, target))
        return lax.ppermute(block, "row", pairs)

    def send(block, name, step):
        count = mesh.shape[name]
        return lax.ppermute(block, name, [(i, (i + step) % count) for i in range(count)])

    def hop(block, pairs):
        return lax.ppermute(
            block, "row", [(a * n_y + y, b * n_y + y) for a, b in pairs for y in range(n_y)]
        )

    def gather_z(block):
        near = hop(block, [(0, 1), (1, 0), (2, 3), (3, 2)])
        across = hop(jnp.stack([near, block]), [(1, 2), (2, 1)])
        outside = hop(across, [(1, 0), (2, 3)])
        return [block, near, across[0] + outside[1], across[1] + outside[0]]

    def gather_y(block):
        return [block] + [send_row(block, 0, -e) for e in range(1, n_y)]

    def gather_name(block, name):
        return [block] + [send(block, name, -s) for s in range(1, mesh.shape[name])]

    def pick(stack, index, axis=0):
        return lax.dynamic_index_in_dim(stack, index, axis, keepdims=False)

    def exchange_row(blocks):
        return lax.all_to_all(blocks, "row", 0, 0, tiled=False)

    def on_device_plain(
        tokens,
        cotangent,
        inner_weight,
        inner_mean,
        inner_square,
        outer_weight,
        outer_mean,
        outer_square,
    ):
        at_m, at_x = lax.axis_index("mem"), lax.axis_index("col")
        token_count, slab = tokens.shape
        width, hidden_local = inner_weight.shape[1:]
        share = hidden_local // n_row

        def gather_line(block):
            return [block] + [send_row(block, -k, 0) for k in range(1, n_z)]

        token_slab = jnp.stack(gather_line(tokens))
        cotangent_slab = jnp.stack(gather_line(cotangent))

        inner_packed = pack(inner_weight).reshape(n_row, share, 2 * width)
        outer_packed = outer_weight.astype(bf16).reshape(n_row, share, width)
        inner_all = exchange_row(inner_packed)
        outer_all = exchange_row(outer_packed)

        def line_to_rows(blocks):
            return jnp.stack(blocks).reshape(n_row * token_count, slab)

        token_slab = line_to_rows(gather_y(token_slab))
        token_slabs = gather_name(token_slab, "col")
        crossed = gather_name(cotangent_slab, "col")
        cotangent_slabs = [line_to_rows(gather_y(c)) for c in crossed]

        def spread(blocks):
            across = [gather_name(b, "mem") for b in blocks]
            return [across[b][a] for a in range(n_mem) for b in range(n_col)]

        token_slabs, cotangent_slabs = spread(token_slabs), spread(cotangent_slabs)

        def slab_at(a, b):
            return ((at_m + a) % n_mem) * n_col + (at_x + b) % n_col

        gate_w, up_w, out_w = [], [], []
        for a in range(n_mem):
            for b in range(n_col):
                at = slab_at(a, b) * n_y
                inner_halves = [pick(inner_all, at + y) for y in range(n_y)]
                outer_halves = [pick(outer_all, at + y) for y in range(n_y)]
                gate_w.append(jnp.concatenate([h[:, :width] for h in inner_halves], axis=1))
                up_w.append(jnp.concatenate([h[:, width:] for h in inner_halves], axis=1))
                out_w.append(jnp.concatenate(outer_halves, axis=1))

        def summed(ws, xs):
            total = contract(ws[0], xs[0], 1, 1)
            for w, x in zip(ws[1:], xs[1:]):
                total = total + contract(w, x, 1, 1)
            return total

        gating = summed(gate_w, token_slabs)
        upward = summed(up_w, token_slabs)
        hidden_back = summed(out_w, cotangent_slabs)
        logistic = jax.nn.sigmoid(gating)
        hidden = (gating * logistic * upward).astype(bf16)
        gating_back = (
            hidden_back * upward * logistic * (1.0 + gating * (1.0 - logistic))
        ).astype(bf16)
        upward_back = (hidden_back * gating * logistic).astype(bf16)

        both = jnp.concatenate([gating_back, upward_back], axis=0)
        partial = [
            contract(both, jnp.concatenate([g, u], axis=0), 0, 0) for g, u in zip(gate_w, up_w)
        ]
        sums = []
        for b in range(n_col):
            total = partial[b]
            for a in range(1, n_mem):
                total = total + send(partial[a * n_col + b].astype(bf16), "mem", a).astype(f32)
            sums.append(total)
        total = sums[0]
        for b in range(1, n_col):
            total = total + send(sums[b].astype(bf16), "col", b).astype(f32)
        total = total.reshape(n_y, n_z, token_count, slab)
        mine = total[0]
        for e in range(1, n_y):
            mine = mine + send_row(total[e].astype(bf16), 0, e).astype(f32)
        token_gradient = mine[0]
        for k in range(1, n_z):
            token_gradient = token_gradient + send_row(mine[k].astype(bf16), k, 0).astype(f32)
        token_gradient = token_gradient.astype(bf16)

        inner_slabs, outer_slabs = [], []
        for t, c in zip(token_slabs, cotangent_slabs):
            g = contract(gating_back, t, 1, 0).astype(bf16)
            u = contract(upward_back, t, 1, 0).astype(bf16)
            o = contract(hidden, c, 1, 0).astype(bf16)
            ranges = [slice(y * width, (y + 1) * width) for y in range(n_y)]
            outer_slabs.append(jnp.stack([o[:, r] for r in ranges]))
            inner_slabs.append(
                jnp.stack([jnp.concatenate([g[:, r], u[:, r]], axis=1) for r in ranges])
            )

        def in_place_order(slabs):
            slabs = jnp.stack(slabs)
            ordered = [
                pick(slabs, ((z // n_col - at_m) % n_mem) * n_col + (z % n_col - at_x) % n_col)
                for z in range(n_z)
            ]
            return jnp.stack(ordered).reshape(n_row, share, slabs.shape[-1])

        outer_back = exchange_row(in_place_order(outer_slabs)).reshape(hidden_local, width)
        inner_back = exchange_row(in_place_order(inner_slabs)).reshape(hidden_local, 2 * width)
        return (
            token_gradient,
            *adam_transposed(inner_weight, inner_mean, inner_square, inner_back),
            *adam_step(outer_weight, outer_mean, outer_square, outer_back.astype(f32)),
        )

    def on_device(
        tokens,
        cotangent,
        inner_weight,
        inner_mean,
        inner_square,
        outer_weight,
        outer_mean,
        outer_square,
    ):
        row = lax.axis_index("row")
        place = jnp.stack([row, lax.axis_index("mem") * n_col + lax.axis_index("col")])
        token_count, slab = tokens.shape
        width, _ = inner_weight.shape[1:]

        def swap_row(block, i):
            return lax.ppermute(block, "row", [(r, r ^ i) for r in range(n_row)])

        def swap(block, name):
            return lax.ppermute(block, name, [(0, 1), (1, 0)])

        def exchange(pieces):
            out = list(pieces)
            for i in range(1, n_row):
                out[i] = swap_row(pieces[i], i)
            return out

        def rows_of(blocks):
            return jnp.stack(blocks).reshape(n_row * token_count, slab)

        token_line = jnp.stack(gather_z(tokens))
        cotangent_line = jnp.stack(gather_z(cotangent))
        pieces = pack_pieces(place, inner_weight, outer_weight.T, n_row)
        pieces = exchange(pieces)

        def spread(line):
            across_y = swap_row(line, 1)
            own = rows_of([line, across_y])
            other = rows_of([swap(line, "col"), swap(across_y, "col")])
            return [own, other, swap(own, "mem"), swap(other, "mem")]

        token_slabs, cotangent_slabs = spread(token_line), spread(cotangent_line)

        *turned, gating_back, upward_back, hidden, weights = project(
            place, pieces, token_slabs, cotangent_slabs, width
        )
        back = gradients(
            place, gating_back, upward_back, hidden, token_slabs, cotangent_slabs, width
        )
        turned, back = lax.optimization_barrier((turned, back))
        back = exchange(back)

        partial = [
            contract(turned[0], weights[j, 0], 1, 0) + contract(turned[1], weights[j, 1], 1, 0)
            for j in range(4)
        ]
        sums = [partial[b] + swap(partial[2 + b].astype(bf16), "mem").astype(f32) for b in range(2)]
        sums = [v.reshape(n_y, n_z, token_count, slab) for v in sums]
        half = n_z // 2
        near = sums[0][:, :half] + swap(sums[1][:, :half].astype(bf16), "col").astype(f32)
        far = jnp.stack([v[1, half:] for v in sums]).astype(bf16)
        far = jnp.stack([v[0, half:] for v in sums]) + swap_row(far, 1).astype(f32)
        near = near[0] + swap_row(near[1].astype(bf16), 1).astype(f32)
        far = far[0] + swap(far[1].astype(bf16), "col").astype(f32)
        blocks = [near[0], near[1], far[0], far[1]]
        token_gradient = blocks[0]
        for k in range(1, n_z):
            token_gradient += swap_row(blocks[k].astype(bf16), n_y * k).astype(f32)
        token_gradient = token_gradient.astype(bf16)

        results = adam_pieces(
            place,
            back,
            (inner_weight, inner_mean, inner_square),
            (outer_weight.T, outer_mean.T, outer_square.T),
        )
        return (token_gradient, *results[:3], *(value.T for value in results[3:]))

    def choose(*arrays):
        width, hidden_local = arrays[2].shape[1:]
        fits = hidden_local % (8 * n_row) == 0 and width % 128 == 64
        if not (fast_mesh(mesh) and fits):
            return on_device_plain(*arrays)
        return on_device(*arrays)

    return choose


def fast_mesh(mesh):
    return tuple(mesh.shape[name] for name in ("mem", "row", "col")) == (2, 8, 2)


def solution(mesh):
    activation = P("row", ("mem", "col"))
    inner = P(None, "row", ("mem", "col"))
    outer = P(("mem", "col"), "row")
    step = jax.shard_map(
        build(mesh),
        mesh=mesh,
        in_specs=(activation, activation, inner, inner, inner, outer, outer, outer),
        out_specs=(activation, inner, inner, inner, outer, outer, outer),
        check_vma=False,
    )
    if not fast_mesh(mesh):
        return step
    return step
```
